256 devices in a mesh: section: 8 (over z_lo, x), dp: 32 (over z_hi, y, core).
Axes of the slice: x: 4, y: 4, z: 8 (z_hi: 4, z_lo: 2; z = z_hi * 2 + z_lo), core: 2. Of those that a mesh axis runs over, the one named last changes fastest.
Arguments:
- ln_input: bfloat16 [8, 4096, 12288], P('section', 'dp'), may hold values from -6 to 6
- ln_grad: bfloat16 [8, 4096, 12288], P('section', 'dp'), may hold values from -6 to 6
- top_grad: bfloat16 [8, 4096, 12288], P('section', 'dp'), may hold values from -6 to 6
- ln_gain: float32 [8, 12288], P('section'), may hold values from 0.1 to 1.9
- hidden: bfloat16 [8, 4096, 64], P('section', 'dp'), may hold values from -8 to 8
- master: float32 [8, 64, 12288], P('section', 'dp'), may hold values from -6 to 6
- moment: float32 [8, 64, 12288], P('section', 'dp'), may hold values from -6 to 6
- second: float32 [8, 64, 12288], P('section', 'dp'), may hold values from 0.1 to 4
Outputs:
- new_master: float32 [8, 64, 12288], P('section', 'dp')
- new_moment: float32 [8, 64, 12288], P('section', 'dp')
- new_second: float32 [8, 64, 12288], P('section', 'dp')
- weights: bfloat16 [8, 64, 12288], P('section')
The draws below stay inside these ranges and needn't reach their ends.
All inputs are finite; a program needn't handle non-finite values.
Results may differ from the reference program's by a relative error of at most 0.0078.
Values may be sent and summed in bfloat16 or wider, within the bound.
No kernel may reach another device: no remote copies, remote signals or barrier semaphores. Data moves between devices by JAX's collectives and lax.ppermute only.
A program may use at most 64 MiB of HBM per device.

```python
import math
import jax
import jax.numpy as jnp
from jax import lax

D = 12288
STEP = 20
TOKENS = 4096
ROWS = 64
N_SECTION = 8


def draw_hidden(key, part):
    keys = jax.random.split(key, 4)
    base = jax.random.normal(keys[0], (N_SECTION, TOKENS, ROWS), jnp.float32)
    position = jnp.arange(ROWS, dtype=jnp.float32) / max(ROWS - 1, 1)
    level = jnp.arange(N_SECTION, dtype=jnp.float32) / max(N_SECTION - 1, 1)
    column = 3.0 ** position * jax.random.uniform(keys[3], (ROWS,), jnp.float32, 0.5, 1.5)
    scaled = base * column[None, None, :] * (3.0 ** level)[:, None, None] / math.sqrt(TOKENS)
    return jnp.clip(scaled, -8.0, 8.0).astype(jnp.bfloat16)


def levels(stream_key, extent, shards, least, top_value):
    factor_of = 1.0
    for dim, parts in shards:
        heights = jax.random.uniform(jax.random.fold_in(jax.random.fold_in(stream_key, 6), dim), (parts,), jnp.float32, least / len(shards), top_value / len(shards))
        factor_of = factor_of * jnp.repeat(jnp.exp(heights), extent[dim] // parts).reshape((-1,) + (1,) * (len(extent) - 1 - dim))
    return factor_of


def noise(stream_key, extent, deviation, bound, cuts=(), kind=jnp.bfloat16):
    level = levels(stream_key, extent, cuts, -0.22, 0.18) if cuts else 1.0
    array = jax.random.normal(stream_key, extent, jnp.float32) * deviation * level
    return jnp.minimum(jnp.maximum(array, -bound), bound).astype(kind)


def setup_inputs(seed: int = 0) -> dict:
    key_of = jax.random.split(jax.random.key(seed), 9)
    return {
        "ln_input": noise(key_of[0], (N_SECTION, TOKENS, D), 1.0, 6.0, ((0, 8), (1, 32))),
        "ln_grad": noise(key_of[1], (N_SECTION, TOKENS, D), 1.0, 6.0, ((0, 8), (1, 32))),
        "top_grad": noise(key_of[2], (N_SECTION, TOKENS, D), 1.0, 6.0, ((0, 8), (1, 32))),
        "ln_gain": jnp.clip(1.0 + 0.18 * jax.random.normal(key_of[3], (N_SECTION, D), jnp.float32), 0.1, 1.9),
        "hidden": draw_hidden(jax.random.fold_in(key_of[8], 71), 0),
        "master": noise(key_of[5], (N_SECTION, ROWS, D), 1.0, 6.0, ((0, 8), (1, 32)), jnp.float32),
        "moment": noise(key_of[6], (N_SECTION, ROWS, D), 1.0, 6.0, ((0, 8), (1, 32)), jnp.float32),
        "second": jnp.clip(jnp.exp(math.log(4.0) - 3.6888794 * jax.random.uniform(key_of[7], (N_SECTION, ROWS, D), jnp.float32) ** levels(key_of[7], (N_SECTION, ROWS, D), ((0, 8), (1, 32)), -0.2, 0.2)), 0.1, 4.0),
    }


def layer_back(ln_input, ln_grad, top_grad, ln_gain):
    values = ln_input.astype(jnp.float32)
    row_mean = lax.optimization_barrier(jnp.mean(values, axis=-1, keepdims=True))
    centred = values - row_mean
    inv_std = 1.0 / jnp.sqrt(lax.optimization_barrier(jnp.mean(centred * centred, axis=-1, keepdims=True)) + 1e-05)
    normed = centred * inv_std
    scaled = ln_grad.astype(jnp.float32) * ln_gain
    inner = scaled - lax.optimization_barrier(jnp.mean(scaled, axis=-1, keepdims=True)) - normed * lax.optimization_barrier(jnp.mean(scaled * normed, axis=-1, keepdims=True))
    return (top_grad.astype(jnp.float32) + inner * inv_std).astype(jnp.bfloat16)

def adam_update(grad, master, moment, second):
    new_moment = 0.9 * moment + 0.1 * grad
    new_second = 0.95 * second + 0.05 * grad * grad
    first_fix = 1.0 - 0.9 ** STEP
    second_fix = 1.0 - 0.95 ** STEP
    update = new_moment / first_fix / (jnp.sqrt(new_second / second_fix) + 1e-08)
    new_master = master - 0.05 * (update + 0.1 * master)
    return (new_master, new_moment, new_second)

def reference(ln_input, ln_grad, top_grad, ln_gain, hidden, master, moment, second):
    final_section = N_SECTION - 1

    def one_section(index):
        upper = jnp.minimum(index + 1, final_section)
        passed = layer_back(ln_input[upper], ln_grad[upper], top_grad[upper], ln_gain[upper])
        received = jnp.where(index == final_section, top_grad[index], passed)
        return lax.dot_general(hidden[index], received, (((0,), (0,)), ((), ())), preferred_element_type=jnp.float32)
    grad = lax.map(one_section, jnp.arange(N_SECTION, dtype=jnp.int32))
    new_master, new_moment, new_second = adam_update(grad, master, moment, second)
    weights = new_master.astype(jnp.bfloat16)
    return (new_master, new_moment, new_second, weights)
```

```python
import jax
import jax.numpy as jnp
from jax import lax
from jax.sharding import Mesh
from jax.sharding import PartitionSpec as P

STEP = 20
DP = ("z", "y", "c")
AXES = ("section", "z", "y", "c")
NZ, NY, NC = 4, 4, 2


def permute(value, sections, route):
    pairs = []
    for s in range(sections):
        for z in range(NZ):
            for y in range(NY):
                for c in range(NC):
                    to = route(s, z, y, c)
                    if to is not None:
                        flat = [((a * NZ + b) * NY + d) * NC + e for a, b, d, e in ((s, z, y, c), to)]
                        pairs.append(tuple(flat))
    return lax.ppermute(value, AXES, pairs)


def slot_rows(rows):
    pair = rows // (NZ * NY * NC)
    slot = lax.broadcasted_iota(jnp.int32, (rows, rows), 0)
    row = lax.broadcasted_iota(jnp.int32, (rows, rows), 1)
    low = slot % pair
    zk = (slot // pair) % NZ
    yj = (slot // (pair * NZ)) % NY
    cx = slot // (pair * NZ * NY)
    far = jnp.where(zk == 0, 2, jnp.where(zk == 1, 1, jnp.where(zk == 2, 3, 0)))
    z = lax.axis_index("z") ^ far
    y = (lax.axis_index("y") + yj) % NY
    c = lax.axis_index("c") ^ 1 ^ cx
    return (row == ((z * NY + y) * NC + c) * pair + low).astype(jnp.bfloat16)


def layer_back(ln_input, ln_grad, top_grad, ln_gain):
    values = ln_input.astype(jnp.float32)
    row_mean = jnp.mean(values, axis=-1, keepdims=True)
    centred = values - row_mean
    inv_std = 1.0 / jnp.sqrt(jnp.mean(centred * centred, axis=-1, keepdims=True) + 1e-05)
    normed = centred * inv_std
    scaled = ln_grad.astype(jnp.float32) * ln_gain[:, None, :]
    inner = (
        scaled
        - jnp.mean(scaled, axis=-1, keepdims=True)
        - normed * jnp.mean(scaled * normed, axis=-1, keepdims=True)
    )
    return (top_grad.astype(jnp.float32) + inner * inv_std).astype(jnp.bfloat16)


def adam_update(grad, master, moment, second):
    new_moment = 0.9 * moment + 0.1 * grad
    new_second = 0.95 * second + 0.05 * grad * grad
    first_fix = 1.0 - 0.9**STEP
    second_fix = 1.0 - 0.95**STEP
    update = new_moment / first_fix / (jnp.sqrt(new_second / second_fix) + 1e-08)
    new_master = master - 0.05 * (update + 0.1 * master)
    return (new_master, new_moment, new_second)


def f32(x):
    return x.astype(jnp.float32)


def b16(x):
    return x.astype(jnp.bfloat16)


def half_reduced(term, sections, only):
    def inside(route):
        return lambda s, z, y, c: route(s, z, y, c) if only is None or s in only else None

    rows = term.shape[0]
    half, chunk = rows // NC, rows // (NC * NY)
    got = permute(b16(term[:half]), sections, inside(lambda s, z, y, c: (s, z, y, 1 - c)))
    chip = term[half:] + f32(got)
    parts = [
        permute(b16(chip[j * chunk : (j + 1) * chunk]), sections, inside(lambda s, z, y, c, j=j: (s, z, (y + j) % NY, c)))
        for j in (2, 1, 3)
    ]
    line = chip[:chunk] + f32(parts[0]) + f32(parts[1]) + f32(parts[2])
    got = permute(b16(line[: chunk // 2]), sections, inside(lambda s, z, y, c: (s, z ^ 1, y, c)))
    return line[chunk // 2 :] + f32(got)


def shards(ln_input, ln_grad, top_grad, ln_gain, hidden, master, moment, second):
    sections = lax.axis_size("section")
    last = sections - 1
    is_last = lax.axis_index("section") == last
    rows, width = hidden.shape[2], master.shape[2]
    own = master.shape[1]
    order = slot_rows(rows)
    own_cols = hidden[0].T
    above = permute(own_cols, sections, lambda s, z, y, c: (s + 1, z, y, c) if s < last else None)

    def term_of(cols, received):
        cols = b16(jnp.dot(order, cols, preferred_element_type=jnp.float32))
        return jnp.dot(cols, received, preferred_element_type=jnp.float32)

    term_last = lax.cond(
        is_last, lambda: term_of(own_cols, top_grad[0]), lambda: jnp.zeros((rows, width), jnp.float32)
    )
    four_last = half_reduced(term_last, sections, (last,))
    got_last = permute(
        b16(four_last[:own]), sections, lambda s, z, y, c: (s, z ^ 3, y, c) if s == last else None
    )
    passed = layer_back(ln_input, ln_grad, top_grad, ln_gain)
    four = half_reduced(term_of(above, passed[0]), sections, None)
    near = permute(b16(four[own:]), sections, lambda s, z, y, c: (s - 1, z, y, c) if s > 0 else None)
    far = permute(b16(four[:own]), sections, lambda s, z, y, c: (s - 1, z ^ 3, y, c) if s > 0 else None)
    grad = jnp.where(is_last, four_last[own:] + f32(got_last), f32(near) + f32(far))
    new_master, new_moment, new_second = adam_update(grad, master[0], moment[0], second[0])
    piece = b16(new_master)
    piece = jnp.concatenate([permute(piece, sections, lambda s, z, y, c: (s, z ^ 3, y, c)), piece])
    piece = jnp.concatenate([permute(piece, sections, lambda s, z, y, c: (s, z ^ 1, y, c)), piece])
    pieces = {
        j: permute(piece, sections, lambda s, z, y, c, j=j: (s, z, (y - j) % NY, c)) for j in (2, 1, 3)
    }
    half = jnp.concatenate([piece, pieces[1], pieces[2], pieces[3]])
    other = permute(half, sections, lambda s, z, y, c: (s, z, y, 1 - c))
    weights = lax.dot_general(
        order, jnp.concatenate([other, half]), (((0,), (0,)), ((), ())), preferred_element_type=jnp.float32
    )
    return (new_master[None], new_moment[None], new_second[None], b16(weights)[None])


def solution(mesh):
    finer = Mesh(mesh.devices.reshape(mesh.shape["section"], NZ, NY, NC), AXES)
    tokens = P("section", DP, None)
    return jax.shard_map(
        shards,
        mesh=finer,
        in_specs=(tokens, tokens, tokens, P("section", None), tokens, tokens, tokens, tokens),
        out_specs=(tokens, tokens, tokens, P("section", None, None)),
        check_vma=False,
    )
```

```python
import jax
import jax.numpy as jnp
from jax import lax
from jax.experimental import pallas as pl
from jax.experimental.pallas import tpu as pltpu
from jax.sharding import Mesh
from jax.sharding import PartitionSpec as P

STEP = 20
DP = ("z", "y", "c")
AXES = ("section", "z", "y", "c")
NZ, NY, NC = 4, 4, 2
LANES = 128
ROWBLOCK = 32
CHUNK = 1024
FAR = (2, 1, 3, 0)


def permute(value, route):
    sections = lax.axis_size("section")
    pairs = []
    for s in range(sections):
        for z in range(NZ):
            for y in range(NY):
                for c in range(NC):
                    to = route(s, z, y, c)
                    flat = [((a % sections * NZ + b) * NY + d % NY) * NC + e for a, b, d, e in ((s, z, y, c), to)]
                    pairs.append(tuple(flat))
    return lax.ppermute(value, AXES, pairs)


def slot_rows(rows):
    pair = rows // (NZ * NY * NC)
    slot = lax.broadcasted_iota(jnp.int32, (rows, rows), 0)
    row = lax.broadcasted_iota(jnp.int32, (rows, rows), 1)
    low = slot % pair
    zk = (slot // pair) % NZ
    yj = (slot // (pair * NZ)) % NY
    cx = slot // (pair * NZ * NY)
    far = jnp.where(zk == 0, FAR[0], jnp.where(zk == 1, FAR[1], jnp.where(zk == 2, FAR[2], FAR[3])))
    z = lax.axis_index("z") ^ far
    y = (lax.axis_index("y") + yj) % NY
    c = lax.axis_index("c") ^ 1 ^ cx
    return (row == ((z * NY + y) * NC + c) * pair + low).astype(jnp.bfloat16)


def f32(x):
    return x.astype(jnp.float32)


def b16(x):
    return x.astype(jnp.bfloat16)


def adam_update(grad, master, moment, second):
    new_moment = 0.9 * moment + 0.1 * grad
    new_second = 0.95 * second + 0.05 * grad * grad
    first_fix = 1.0 - 0.9**STEP
    second_fix = 1.0 - 0.95**STEP
    update = new_moment / first_fix / (jnp.sqrt(new_second / second_fix) + 1e-08)
    new_master = master - 0.05 * (update + 0.1 * master)
    return (new_master, new_moment, new_second)


def lane_sum(x):
    parts = [x[:, k * LANES : (k + 1) * LANES] for k in range(x.shape[1] // LANES)]
    while len(parts) > 1:
        parts = [a + b for a, b in zip(parts[::2], parts[1::2])] + ([parts[-1]] if len(parts) % 2 else [])
    return parts[0]


def load_kernel(wanted, t_hbm, cols_hbm, a_hbm, b_hbm, c_hbm, order, t, a, b, c, away, own, cols, sems, small):
    half, width = away.shape
    parts = sems.shape[0]
    copies = []
    for i in range(parts):
        at = pl.ds(i * (width // parts), width // parts)
        copies.append(pltpu.make_async_copy(t_hbm.at[0, :, at], t.at[:, at], sems.at[i]))
    for i, (src, dst) in enumerate(((cols_hbm, cols), (a_hbm, a), (b_hbm, b), (c_hbm, c))):
        copies.append(pltpu.make_async_copy(src, dst, small.at[i]))
    for copy in copies:
        copy.start()
    for copy in copies:
        copy.wait()

    @pl.when(wanted[0] > 0)
    def _():
        slots = b16(jnp.dot(order[...], cols[...], preferred_element_type=jnp.float32))
        for i in range(width // CHUNK):
            at = pl.ds(i * CHUNK, CHUNK)
            term = b16(jnp.dot(slots, t[:, at], preferred_element_type=jnp.float32))
            away[:, at] = term[:half]
            own[:, at] = term[half:]


def stats_kernel(x_hbm, g_hbm, gain, inv_b, k1_b, k0_b, x, g, sems):
    tokens, width = x.shape
    blocks = tokens // ROWBLOCK
    copies = {}
    for b in range(blocks):
        rows = pl.ds(b * ROWBLOCK, ROWBLOCK)
        for k, (src, dst) in enumerate(((x_hbm, x), (g_hbm, g))):
            copies[k, b] = pltpu.make_async_copy(src.at[0, rows], dst.at[rows], sems.at[k, b])
            copies[k, b].start()
    part = 2048
    for b in range(blocks):
        rows = pl.ds(b * ROWBLOCK, ROWBLOCK)
        zero = jnp.zeros((ROWBLOCK, LANES), jnp.float32)
        copies[0, b].wait()

        def first(i, total):
            at = pl.ds(pl.multiple_of(i * part, part), part)
            return total + lane_sum(f32(x[rows, at]))

        mean = jnp.sum(lax.fori_loop(0, width // part, first, zero), axis=1, keepdims=True) / width
        copies[1, b].wait()
        mean_b = jnp.broadcast_to(mean, (ROWBLOCK, LANES))

        def second(i, totals):
            square, scale, cross = totals
            at0 = pl.multiple_of(i * (part // 2), part // 2)
            for k in range(part // 2 // LANES):
                at = pl.ds(at0 + k * LANES, LANES)
                centred = f32(x[rows, at]) - mean_b
                scaled = f32(g[rows, at]) * gain[:, at]
                square = square + centred * centred
                scale = scale + scaled
                cross = cross + scaled * centred
            return square, scale, cross

        square, scale, cross = lax.fori_loop(0, width // (part // 2), second, (zero, zero, zero))
        inv = 1.0 / jnp.sqrt(jnp.sum(square, axis=1, keepdims=True) / width + 1e-05)
        mean_scaled = jnp.sum(scale, axis=1, keepdims=True) / width
        k1 = jnp.sum(cross, axis=1, keepdims=True) / width * inv * inv * inv
        inv_b[rows, :] = jnp.broadcast_to(inv, (ROWBLOCK, LANES))
        k1_b[rows, :] = jnp.broadcast_to(k1, (ROWBLOCK, LANES))
        k0_b[rows, :] = jnp.broadcast_to(mean * k1 - inv * mean_scaled, (ROWBLOCK, LANES))


def norm_term_kernel(gain, inv_b, k1_b, k0_b, x, g, t, order, cols, away, own, passed):
    tokens, width = x.shape
    half = away.shape[0]
    chunks = width // CHUNK

    slots = b16(jnp.dot(order[...], cols[...], preferred_element_type=jnp.float32))

    def fill(i):
        lanes = [pl.ds(i * CHUNK + k * LANES, LANES) for k in range(CHUNK // LANES)]
        gains = [gain[:, at] for at in lanes]
        for r in range(tokens // 16):
            rows = slice(16 * r, 16 * r + 16)
            inv, k1, k0 = inv_b[rows, :], k1_b[rows, :], k0_b[rows, :]
            for k, at in enumerate(lanes):
                inner = f32(g[rows, at]) * gains[k] * inv - f32(x[rows, at]) * k1 + k0
                passed[i % 2, rows, k * LANES : (k + 1) * LANES] = b16(f32(t[rows, at]) + inner)

    def multiply(i):
        at = pl.ds(i * CHUNK, CHUNK)
        term = b16(jnp.dot(slots, passed[i % 2], preferred_element_type=jnp.float32))
        away[:, at] = term[:half]
        own[:, at] = term[half:]

    fill(0)
    for i in range(chunks):
        if i + 1 < chunks:
            fill(i + 1)
        multiply(i)


VMEM = pl.BlockSpec(memory_space=pltpu.VMEM)
HBM = pl.BlockSpec(memory_space=pltpu.HBM)


def loaded_term(wanted, top_grad, cols, state, order):
    _, tokens, width = top_grad.shape
    half = cols.shape[0] // 2
    return pl.pallas_call(
        load_kernel,
        out_shape=[jax.ShapeDtypeStruct((tokens, width), jnp.bfloat16)]
        + [jax.ShapeDtypeStruct(x.shape, x.dtype) for x in state]
        + [jax.ShapeDtypeStruct((half, width), jnp.bfloat16)] * 2,
        in_specs=[pl.BlockSpec(memory_space=pltpu.SMEM), HBM, HBM, HBM, HBM, HBM, VMEM],
        out_specs=[VMEM] * 6,
        scratch_shapes=[
            pltpu.VMEM(cols.shape, cols.dtype), pltpu.SemaphoreType.DMA((4,)), pltpu.SemaphoreType.DMA((4,)),
        ],
        compiler_params=pltpu.CompilerParams(vmem_limit_bytes=56 * 2**20),
        cost_estimate=pl.CostEstimate(flops=128 * tokens * width, bytes_accessed=2 * tokens * width, transcendentals=0),
    )(wanted, top_grad, cols, *state, order)


def norm_stats(ln_input, ln_grad, ln_gain):
    _, tokens, width = ln_input.shape
    return pl.pallas_call(
        stats_kernel,
        out_shape=[jax.ShapeDtypeStruct((tokens, LANES), jnp.float32)] * 3
        + [jax.ShapeDtypeStruct((tokens, width), jnp.bfloat16)] * 2,
        in_specs=[HBM, HBM, VMEM],
        out_specs=[VMEM] * 5,
        scratch_shapes=[pltpu.SemaphoreType.DMA((2, tokens // ROWBLOCK))],
        compiler_params=pltpu.CompilerParams(vmem_limit_bytes=50 * 2**20),
        cost_estimate=pl.CostEstimate(flops=256 * tokens * width, bytes_accessed=4 * tokens * width, transcendentals=0),
    )(ln_input, ln_grad, ln_gain)


def norm_term(ln_gain, stats, order, cols):
    tokens, width = stats[3].shape
    half = cols.shape[0] // 2
    return pl.pallas_call(
        norm_term_kernel,
        out_shape=[jax.ShapeDtypeStruct((half, width), jnp.bfloat16)] * 2,
        in_specs=[VMEM] * 9,
        out_specs=[VMEM, VMEM],
        scratch_shapes=[pltpu.VMEM((2, tokens, CHUNK), jnp.bfloat16)],
        compiler_params=pltpu.CompilerParams(vmem_limit_bytes=20 * 2**20),
        cost_estimate=pl.CostEstimate(flops=128 * tokens * width, bytes_accessed=6 * tokens * width, transcendentals=0),
    )(ln_gain, *stats, order, cols)


def rows_kernel(order, *refs):
    pieces, weights, staged, sems = refs[:-3], refs[-3], refs[-2], refs[-1]
    width = weights.shape[1]
    part = 2048
    copies = []
    for i in range(width // part):
        at = pl.ds(i * part, part)
        slots = jnp.concatenate([piece[:, at] for piece in pieces])
        picked = lax.dot_general(order[...], slots, (((0,), (0,)), ((), ())), preferred_element_type=jnp.float32)
        staged[:, at] = b16(picked)
        copies.append(pltpu.make_async_copy(staged.at[:, at], weights.at[:, at], sems.at[i]))
        copies[-1].start()
    for copy in copies:
        copy.wait()


def rows_in_order(order, pieces):
    rows, width = order.shape[0], pieces[0].shape[1]
    return pl.pallas_call(
        rows_kernel,
        out_shape=jax.ShapeDtypeStruct((rows, width), jnp.bfloat16),
        in_specs=[VMEM] * (1 + len(pieces)),
        out_specs=HBM,
        scratch_shapes=[pltpu.VMEM((rows, width), jnp.bfloat16), pltpu.SemaphoreType.DMA((width // 2048,))],
        compiler_params=pltpu.CompilerParams(vmem_limit_bytes=16 * 2**20),
        cost_estimate=pl.CostEstimate(flops=64 * rows * width, bytes_accessed=4 * rows * width, transcendentals=0),
    )(order, *pieces)


def chip_sum(away, own):
    return f32(own) + f32(permute(away, lambda s, z, y, c: (s, z, y, 1 - c)))


def y_parts(chip):
    chunk = chip.shape[0] // NY
    parts = [chip[:chunk]]
    for j in (2, 1, 3):
        part = b16(chip[j * chunk : (j + 1) * chunk])
        parts.append(permute(part, lambda s, z, y, c, j=j: (s, z, y + j, c)))
    return parts


def summed(parts):
    return f32(parts[0]) + f32(parts[1]) + f32(parts[2]) + f32(parts[3])


def z_sum(line):
    chunk = line.shape[0] // NZ
    total = line[3 * chunk :]
    for k in range(3):
        part = b16(line[k * chunk : (k + 1) * chunk])
        got = permute(part, lambda s, z, y, c, k=k: (s, z ^ FAR[k], y, c))
        total = total + f32(got)
    return total


def update(ln_input, ln_grad, top_grad, ln_gain, hidden, master, moment, second):
    is_last = lax.axis_index("section") == lax.axis_size("section") - 1
    rows, width = hidden.shape[2], master.shape[2]
    own = master.shape[1]
    order = slot_rows(rows)
    own_cols = hidden[0].T
    above = permute(own_cols, lambda s, z, y, c: (s + 1, z, y, c))

    loaded, master, moment, second, away_last, own_last = loaded_term(
        is_last.astype(jnp.int32)[None], top_grad, own_cols, (master, moment, second), order
    )
    other_last = permute(away_last, lambda s, z, y, c: (s, z, y, 1 - c))
    stats = norm_stats(ln_input, ln_grad, ln_gain)

    def main_parts():
        halves = norm_term(ln_gain, (*stats, loaded), order, above)
        return y_parts(chip_sum(*halves))

    def last_section():
        parts_last = y_parts(f32(own_last) + f32(other_last))
        mine, *others = main_parts()
        mine, *parts_last = lax.optimization_barrier((mine, *parts_last))
        grad = z_sum(summed(parts_last))
        return b16(summed([mine, *others])), grad

    def other_section():
        return b16(summed(main_parts())), jnp.zeros((own, width), jnp.float32)

    line, grad_last = lax.cond(is_last, last_section, other_section)
    grad = jnp.zeros((own, width), jnp.float32)
    for k in range(NZ):
        grad = grad + f32(
            permute(line[k * own : (k + 1) * own], lambda s, z, y, c, k=k: (s - 1, z ^ FAR[k], y, c))
        )
    grad = jnp.where(is_last, grad_last, grad)
    new_master, new_moment, new_second = adam_update(grad, master[0], moment[0], second[0])
    piece = b16(new_master)
    piece = jnp.concatenate([permute(piece, lambda s, z, y, c: (s, z ^ 3, y, c)), piece])
    piece = jnp.concatenate([permute(piece, lambda s, z, y, c: (s, z ^ 1, y, c)), piece])

    def swap(x):
        return permute(x, lambda s, z, y, c: (s, z, y, 1 - c))

    half = {0: piece}
    for j in (2, 1, 3):
        half[j] = permute(piece, lambda s, z, y, c, j=j: (s, z, y - j, c))
    other = {j: swap(half[j]) for j in (0, 2, 1, 3)}
    weights = rows_in_order(order, [other[j] for j in range(NY)] + [half[j] for j in range(NY)])
    return (new_master[None], new_moment[None], new_second[None], weights[None])


def solution(mesh):
    finer = Mesh(mesh.devices.reshape(mesh.shape["section"], NZ, NY, NC), AXES)
    tokens = P("section", DP, None)
    return jax.shard_map(
        update,
        mesh=finer,
        in_specs=(tokens, tokens, tokens, P("section", None), tokens, tokens, tokens, tokens),
        out_specs=(tokens, tokens, tokens, P("section", None, None)),
        check_vma=False,
    )
```
